32 devices in a mesh: kpt: 4 (over y, x), pw: 8 (over z, core).
Axes of the slice: x: 2, y: 2, z: 4, core: 2. Of those that a mesh axis runs over, the one named last changes fastest.
Arguments:
- energies: float32 [16, 512], P('kpt', 'pw'), may hold values from 0.5 to 3
- current: float32 [2, 16, 512], P(None, 'kpt', 'pw'), may hold values from -40 to 40
- previous: float32 [2, 16, 512], P(None, 'kpt', 'pw'), may hold values from -6 to 6
- previous_beta: float32 [2], replicated, may hold values from 0.5 to 2
- pair_left: bfloat16 [16, 512, 4096], P('kpt', None, 'pw'), may hold values from -0.09375 to 0.09375
- pair_right: bfloat16 [16, 512, 4096], P('kpt', None, 'pw'), may hold values from -0.25 to 0.25
- screened: bfloat16 [16, 4096, 4096], P('kpt', 'pw'), may hold values from -0.0234375 to 0.0234375
- momentum_index: int32 [16, 16], replicated, may hold values from 0 to 15, each once within a row
Outputs:
- last_vector: float32 [2, 16, 512], P(None, 'kpt', 'pw')
- prior_vector: float32 [2, 16, 512], P(None, 'kpt', 'pw')
- alpha_terms: float32 [2, 3], replicated
- beta_terms: float32 [2, 3], replicated
The draws below stay inside these ranges and needn't reach their ends.
Inputs may be any that keep to these rules, and one draw needn't show every extreme that they name: Each row of momentum_index names every index from 0 to 15 once.
All inputs are finite; a program needn't handle non-finite values.
Results may differ from the reference program's by a relative error of at most 0.003.
Values may be sent and summed in bfloat16 or wider, within the bound.
A program may use at most 128 MiB of HBM per device.

```python
import math
import jax
import jax.numpy as jnp
from jax import lax

NK = 16
NC = 512
NG = 4096
NVEC = 2
STEPS = 3


def draw_current(key, part):
    normal_part = jnp.clip(jax.random.normal(key, (NVEC, NK, NC), jnp.float32), -4.0, 4.0)
    kpoint_frac = jnp.arange(NK, dtype=jnp.float32) / NK
    band_frac = jnp.arange(NC, dtype=jnp.float32) / NC
    values = normal_part
    kpoint_scale = 10.0 ** (kpoint_frac - 0.5)
    band_scale = 10.0 ** (band_frac - 0.5)
    return values * kpoint_scale[None, :, None] * band_scale[None, None, :]


def block_scale(stream_key, shape, pieces, smallest, high):
    def one(axis_at, blocks):
        steps = jax.random.uniform(jax.random.fold_in(jax.random.fold_in(stream_key, 6), axis_at), (blocks,), jnp.float32, smallest / len(pieces), high / len(pieces))
        return jnp.repeat(jnp.exp(steps), shape[axis_at] // blocks).reshape((-1,) + (1,) * (len(shape) - axis_at - 1))

    factor_of = one(*pieces[0])
    for cut in pieces[1:]:
        factor_of = factor_of * one(*cut)
    return factor_of


def centred(stream_key, dims, scale, reach, cuts=(), held_as=jnp.bfloat16):
    values = jax.random.normal(stream_key, dims, jnp.float32) * scale
    if len(cuts) > 0:
        values = block_scale(stream_key, dims, cuts, -0.22, 0.18) * values
    return jnp.clip(values, min=-reach, max=reach).astype(held_as)


def setup_inputs(seed: int = 0) -> dict:
    key_list = jax.random.split(jax.random.key(seed), 9)
    energies = jnp.clip(0.5 + 2.5 * jax.random.uniform(key_list[0], (NK, NC), jnp.float32) ** block_scale(key_list[0], (NK, NC), ((0, 4), (1, 8)), -0.2, 0.2), 0.5, 3.0)
    current = draw_current(jax.random.fold_in(key_list[8], 71), 0)
    previous = centred(key_list[2], (NVEC, NK, NC), 1.0, 6.0, ((1, 4), (2, 8)), jnp.float32)
    previous_beta = jnp.clip(jnp.exp(jax.random.uniform(key_list[3], (NVEC,), jnp.float32, math.log(0.5), math.log(2.0))), 0.5, 2.0)
    pair_left = centred(key_list[4], (NK, NC, NG), NG ** -0.5, 0.09375, ((0, 4), (2, 8)))
    pair_right = centred(key_list[5], (NK, NC, NG), NC ** -0.5, 0.25, ((0, 4), (2, 8)))
    screened = centred(key_list[6], (NK, NG, NG), (NK * NG) ** -0.5, 0.0234375, ((0, 4), (1, 8)))
    momentum_index = jax.vmap(lambda own: jax.random.permutation(own, NK))(jax.random.split(key_list[7], NK)).reshape((NK, NK)).astype(jnp.int32)
    return dict(energies=energies, current=current, previous=previous, previous_beta=previous_beta, pair_left=pair_left, pair_right=pair_right, screened=screened, momentum_index=momentum_index)


epsilon = 1e-06

def reference(energies, current, previous, previous_beta, pair_left, pair_right, screened, momentum_index):
    entries = NK * NC
    left_float = pair_left.astype(jnp.float32)
    right_float = pair_right.astype(jnp.float32)
    vector = current
    earlier = previous
    beta_before = previous_beta
    alpha_list = []
    beta_list = []
    for turn_index in range(STEPS):
        rounded = vector.astype(jnp.bfloat16)
        density = jnp.einsum('kcg,vkc->kvg', right_float, rounded.astype(jnp.float32), precision=lax.Precision.HIGHEST).astype(jnp.bfloat16)
        columns = density.reshape(NK * NVEC, NG).T

        def add_transfer(running, qpoint):
            images = jnp.dot(screened[qpoint], columns, preferred_element_type=jnp.float32).reshape(NG, NK, NVEC)
            selector = (momentum_index == qpoint).astype(jnp.float32)
            return (running + jnp.einsum('jk,gkv->jvg', selector, images, precision=lax.Precision.HIGHEST), None)
        potential, unused = lax.scan(add_transfer, jnp.zeros((NK, NVEC, NG), jnp.float32), jnp.arange(NK, dtype=jnp.int32))
        potential_bf = potential.astype(jnp.bfloat16)
        direct = jnp.einsum('kcg,kvg->vkc', left_float, potential_bf.astype(jnp.float32), precision=lax.Precision.HIGHEST)
        applied = energies[None] * vector - direct - beta_before[:, None, None] * earlier
        alpha_now = lax.optimization_barrier(jnp.sum(vector * applied, axis=(1, 2))) / entries
        residual = applied - alpha_now[:, None, None] * vector
        beta_now = jnp.sqrt(lax.optimization_barrier(jnp.sum(residual * residual, axis=(1, 2))) / entries + epsilon)
        earlier = vector
        vector = residual / beta_now[:, None, None]
        beta_before = beta_now
        alpha_list.append(alpha_now)
        beta_list.append(beta_now)
    return (vector, earlier, jnp.stack(alpha_list, axis=1), jnp.stack(beta_list, axis=1))
```

```python
import functools

import jax
import jax.numpy as jnp
from jax import lax
from jax.experimental import pallas as pl
from jax.experimental.pallas import tpu as pltpu
from jax.sharding import PartitionSpec as P

STEPS = 3
LANES = 128

epsilon = 1e-06


def partner(me, i, n):
    i = jnp.int32(i)
    out = jnp.int32(0)
    bit = 1
    while bit < n:
        out = out + lax.rem(lax.div(me, bit) + lax.div(i, bit), 2) * bit
        bit *= 2
    return out


def exchange(buf, axis, n, me, i, send_sem, recv_sem, src=None):
    return pltpu.make_async_remote_copy(
        src_ref=buf.at[me] if src is None else src,
        dst_ref=buf.at[me],
        send_sem=send_sem.at[i],
        recv_sem=recv_sem.at[i],
        device_id={axis: partner(me, i, n)},
        device_id_type=pl.DeviceIdType.MESH,
    )


def arrival(buf, axis, n, me, i, send_sem, recv_sem):
    slot = partner(me, i, n)
    return pltpu.make_async_remote_copy(
        src_ref=buf.at[slot],
        dst_ref=buf.at[slot],
        send_sem=send_sem.at[i],
        recv_sem=recv_sem.at[i],
        device_id={axis: slot},
        device_id_type=pl.DeviceIdType.MESH,
    )


def kernel(
    dims,
    packed_ref, beta_ref, choose_ref, right_hbm, left_hbm, screened_hbm,
    vec_ref, early_ref, coef_ref,
    right, left, screened, packs, first, later, final, dens, images, held, fields, directs,
    dfull, applied_ref, energy_ref, acc,
    right_sem, left_sem, screened_sem,
    pack_s, pack_r, kdens_s, kdens_r, gdens_s, gdens_r, field_s, field_r,
    direct_s, direct_r, final_s, final_r,
):
    nkp, npw, kl, nv, bands, gs = dims
    rows = kl * nv
    total = rows * nkp
    entries = total // nv * bands
    kme = lax.axis_index("kpt")
    pme = lax.axis_index("pw")

    right_copy = pltpu.make_async_copy(right_hbm, right, right_sem)
    left_copy = pltpu.make_async_copy(left_hbm, left, left_sem)

    def screened_copy(i):
        chunk = partner(pme, i, npw)
        start = pl.multiple_of(chunk * gs, gs)
        return pltpu.make_async_copy(
            screened_hbm.at[:, :, pl.ds(start, gs)], screened.at[chunk], screened_sem.at[i]
        )

    right_copy.start()
    for i in range(npw):
        screened_copy(i).start()
    left_copy.start()

    barrier = pltpu.get_barrier_semaphore()
    for axis, n, me in (("kpt", nkp, kme), ("pw", npw, pme)):
        for i in range(1, n):
            pl.semaphore_signal(
                barrier, inc=1, device_id={axis: partner(me, i, n)},
                device_id_type=pl.DeviceIdType.MESH,
            )
    packs[pme] = packed_ref[...]
    pl.semaphore_wait(barrier, nkp - 1 + npw - 1)

    pending = []

    def send_all(buf, axis, n, me, ssem, rsem):
        for i in range(1, n):
            copy = exchange(buf, axis, n, me, i, ssem, rsem)
            copy.start()
            pending.append(copy)

    def wait_all(buf, axis, n, me, ssem, rsem):
        for i in range(1, n):
            arrival(buf, axis, n, me, i, ssem, rsem).wait_recv()

    send_all(packs, "pw", npw, pme, pack_s, pack_r)
    wait_all(packs, "pw", npw, pme, pack_s, pack_r)

    per = npw * LANES // bands
    whole = jnp.concatenate(
        [sum(packs[m * per + j] for j in range(per)) for m in range(bands // LANES)], axis=1
    )
    vec_ref[...] = whole[:rows]
    early_ref[...] = whole[rows : 2 * rows]
    energy_ref[...] = whole[2 * rows :]
    coef_ref[...] = jnp.zeros_like(coef_ref)

    row_g = lax.broadcasted_iota(jnp.int32, (rows, gs), 0) // nv
    row_c = lax.broadcasted_iota(jnp.int32, (rows, bands), 0) // nv
    row_v = lax.rem(lax.broadcasted_iota(jnp.int32, (rows, LANES), 0), nv)
    lane = lax.broadcasted_iota(jnp.int32, (rows, LANES), 1)

    def densities(x):
        high = x.astype(jnp.bfloat16).astype(jnp.float32)
        both = jnp.concatenate([high, x - high], axis=0).astype(jnp.bfloat16)
        top = jnp.zeros((rows, gs), jnp.float32)
        low = jnp.zeros((rows, gs), jnp.float32)
        for k in range(kl):
            res = jnp.dot(both, right[k], preferred_element_type=jnp.float32)
            top = jnp.where(row_g == k, res[:rows], top)
            low = jnp.where(row_g == k, res[rows:], low)
        return top, low

    def sums_tile(vec, applied):
        cross = jnp.sum(vec * applied, axis=1, keepdims=True)
        square = jnp.sum(applied * applied, axis=1, keepdims=True)
        own = jnp.sum(vec * vec, axis=1, keepdims=True)
        return jnp.where(lane == 0, cross, jnp.where(lane == 1, square, own))

    def coefficients(tile, turn):
        sums = jnp.zeros_like(tile)
        for v in range(nv):
            chain = jnp.sum(jnp.where(row_v == v, tile, 0.0), axis=0, keepdims=True)
            sums = jnp.where(row_v == v, chain, sums)
        alpha = sums[:, 0:1] / entries
        mean = sums[:, 1:2] / entries - 2.0 * alpha * alpha + alpha * alpha * (sums[:, 2:3] / entries)
        beta = jnp.sqrt(mean + epsilon)
        coef = jnp.where(lane == turn, alpha, coef_ref[...])
        coef_ref[...] = jnp.where(lane == STEPS + turn, beta, coef)
        return alpha, beta

    def advance(alpha, beta):
        vec = vec_ref[...]
        early_ref[...] = vec
        vec_ref[...] = (applied_ref[...] - alpha * vec) / beta

    beta_before = beta_ref[:, 0:1]
    right_copy.wait()
    for turn in range(STEPS):
        if turn == 0:
            top, low = densities(vec_ref[...])
            first[kme] = jnp.concatenate([top, top + low], axis=1)
            send_all(first, "kpt", nkp, kme, kdens_s.at[turn], kdens_r.at[turn])
            wait_all(first, "kpt", nkp, kme, kdens_s.at[turn], kdens_r.at[turn])
            blocks = []
            for s in range(nkp):
                blocks.append(first[s][:, :gs])
                dfull[s] = first[s][:, gs:]
        else:
            applied = applied_ref[...]
            top, low = densities(applied)
            mine = later.at[turn - 1]
            mine[kme] = jnp.concatenate([top + low, sums_tile(vec_ref[...], applied)], axis=1)
            send_all(mine, "kpt", nkp, kme, kdens_s.at[turn], kdens_r.at[turn])
            wait_all(mine, "kpt", nkp, kme, kdens_s.at[turn], kdens_r.at[turn])
            alpha, beta = coefficients(sum(mine[s][:, gs:] for s in range(nkp)), turn - 1)
            blocks = []
            for s in range(nkp):
                block = (mine[s][:, :gs] - alpha * dfull[s]) / beta
                dfull[s] = block
                blocks.append(block)
        gathered = dens.at[turn]
        gathered[pme] = jnp.concatenate(blocks, axis=0).astype(jnp.bfloat16)
        send_all(gathered, "pw", npw, pme, gdens_s.at[turn], gdens_r.at[turn])
        if turn > 0:
            advance(alpha, beta)
            beta_before = beta
        acc[...] = jnp.zeros_like(acc)

        def chunk_step(i, carry):
            @pl.when(i > 0)
            def _():
                arrival(
                    gathered, "pw", npw, pme, i, gdens_s.at[turn], gdens_r.at[turn]
                ).wait_recv()

            if turn == 0:
                screened_copy(i).wait()
            chunk = partner(pme, i, npw)
            picked = jnp.dot(
                choose_ref[...], gathered[chunk], preferred_element_type=jnp.float32
            ).astype(jnp.bfloat16)
            part = acc[...]
            for q in range(kl):
                part = part + lax.dot_general(
                    picked[q * total : (q + 1) * total],
                    screened[chunk, q],
                    (((1,), (1,)), ((), ())),
                    preferred_element_type=jnp.float32,
                )
            acc[...] = part
            return carry

        lax.fori_loop(0, npw, chunk_step, 0)
        out = held.at[turn]
        for s in range(nkp):
            out[s] = acc[s * rows : (s + 1) * rows, :]
        mine = fields.at[turn]
        for i in range(1, nkp):
            copy = exchange(
                mine, "kpt", nkp, kme, i, field_s.at[turn], field_r.at[turn],
                src=out.at[partner(kme, i, nkp)],
            )
            copy.start()
            pending.append(copy)
        mine[kme] = out[kme]
        if turn == 0:
            left_copy.wait()
        wait_all(mine, "kpt", nkp, kme, field_s.at[turn], field_r.at[turn])
        field = sum(mine[s] for s in range(nkp)).astype(jnp.bfloat16)
        part = jnp.zeros((rows, bands), jnp.float32)
        for k in range(kl):
            res = lax.dot_general(
                field, left[k], (((1,), (1,)), ((), ())), preferred_element_type=jnp.float32
            )
            part = jnp.where(row_c == k, res, part)
        mine = directs.at[turn]
        mine[pme] = part
        send_all(mine, "pw", npw, pme, direct_s.at[turn], direct_r.at[turn])
        wait_all(mine, "pw", npw, pme, direct_s.at[turn], direct_r.at[turn])
        direct = sum(mine[s] for s in range(npw))
        applied_ref[...] = (
            energy_ref[...] * vec_ref[...] - direct - beta_before * early_ref[...]
        )
    final[kme] = sums_tile(vec_ref[...], applied_ref[...])
    send_all(final, "kpt", nkp, kme, final_s, final_r)
    wait_all(final, "kpt", nkp, kme, final_s, final_r)
    alpha, beta = coefficients(sum(final[s] for s in range(nkp)), STEPS - 1)
    advance(alpha, beta)
    for copy in pending:
        copy.wait_send()


def on_device(
    nkp, npw,
    energies, current, previous, previous_beta, pair_left, pair_right, screened, momentum_index
):
    nv, kl, width = current.shape
    bands = pair_left.shape[1]
    gs = pair_left.shape[2]
    qcount = screened.shape[0]
    rows = kl * nv
    total = rows * nkp
    kme = lax.axis_index("kpt")
    pme = lax.axis_index("pw")
    to_rows = lambda a: jnp.transpose(a, (1, 0, 2)).reshape(rows, width)
    levels = jnp.broadcast_to(energies[:, None], (kl, nv, width)).reshape(rows, width)
    block = jnp.concatenate([to_rows(current), to_rows(previous), levels], axis=0)
    per = LANES // width
    spot = (jnp.arange(per) == pme % per)[None, :, None]
    packed = jnp.where(spot, block[:, None, :], 0.0).reshape(3 * rows, LANES)
    beta_rows = jnp.broadcast_to(jnp.tile(previous_beta, kl)[:, None], (rows, LANES))
    qpoints = kme * qcount + jnp.arange(qcount, dtype=jnp.int32)
    select = momentum_index[None] == qpoints[:, None, None]
    same = jnp.eye(nv, dtype=bool)
    choose = (select[:, :, None, :, None] & same[None, None, :, None, :]).astype(jnp.bfloat16)
    choose = choose.reshape(qcount * total, total)

    f32, bf16 = jnp.float32, jnp.bfloat16
    vmem = pl.BlockSpec(memory_space=pltpu.VMEM)
    hbm = pl.BlockSpec(memory_space=pl.ANY)
    dma = pltpu.SemaphoreType.DMA
    vec, early, coef = pl.pallas_call(
        functools.partial(kernel, (nkp, npw, kl, nv, bands, gs)),
        out_shape=(
            jax.ShapeDtypeStruct((rows, bands), f32),
            jax.ShapeDtypeStruct((rows, bands), f32),
            jax.ShapeDtypeStruct((rows, LANES), f32),
        ),
        in_specs=[vmem, vmem, vmem, hbm, hbm, hbm],
        out_specs=(vmem, vmem, vmem),
        scratch_shapes=[
            pltpu.VMEM((kl, bands, gs), bf16),
            pltpu.VMEM((kl, bands, gs), bf16),
            pltpu.VMEM((npw, qcount, gs, gs), bf16),
            pltpu.VMEM((npw, 3 * rows, LANES), f32),
            pltpu.VMEM((nkp, rows, 2 * gs), f32),
            pltpu.VMEM((STEPS - 1, nkp, rows, gs + LANES), f32),
            pltpu.VMEM((nkp, rows, LANES), f32),
            pltpu.VMEM((STEPS, npw, total, gs), bf16),
            pltpu.VMEM((rows, LANES), f32),
            pltpu.VMEM((STEPS, nkp, rows, gs), f32),
            pltpu.VMEM((STEPS, nkp, rows, gs), f32),
            pltpu.VMEM((STEPS, npw, rows, bands), f32),
            pltpu.VMEM((nkp, rows, gs), f32),
            pltpu.VMEM((rows, bands), f32),
            pltpu.VMEM((rows, bands), f32),
            pltpu.VMEM((total, gs), f32),
            dma, dma, dma((npw,)),
            dma((npw,)), dma((npw,)),
            dma((STEPS, nkp)), dma((STEPS, nkp)),
            dma((STEPS, npw)), dma((STEPS, npw)),
            dma((STEPS, nkp)), dma((STEPS, nkp)),
            dma((STEPS, npw)), dma((STEPS, npw)),
            dma((nkp,)), dma((nkp,)),
        ],
        compiler_params=pltpu.CompilerParams(
            collective_id=0, has_side_effects=True, vmem_limit_bytes=48 * 1024 * 1024
        ),
    )(packed, beta_rows, choose, pair_right, pair_left, screened)

    def own(a):
        a = jnp.transpose(a.reshape(kl, nv, bands), (1, 0, 2))
        return lax.dynamic_slice_in_dim(a, pme * width, width, 2)

    return own(vec), own(early), coef[:nv, :STEPS], coef[:nv, STEPS : 2 * STEPS]


def solution(mesh):
    return jax.shard_map(
        functools.partial(on_device, mesh.shape["kpt"], mesh.shape["pw"]),
        mesh=mesh,
        in_specs=(
            P("kpt", "pw"),
            P(None, "kpt", "pw"),
            P(None, "kpt", "pw"),
            P(),
            P("kpt", None, "pw"),
            P("kpt", None, "pw"),
            P("kpt", "pw", None),
            P(),
        ),
        out_specs=(P(None, "kpt", "pw"), P(None, "kpt", "pw"), P(), P()),
        check_vma=False,
    )
```

```python
import functools

import jax
import jax.numpy as jnp
from jax import lax
from jax.experimental import pallas as pl
from jax.experimental.pallas import tpu as pltpu
from jax.sharding import PartitionSpec as P

STEPS = 3
LANES = 128

epsilon = 1e-06


def partner(me, i, n):
    i = jnp.int32(i)
    out = jnp.int32(0)
    bit = 1
    while bit < n:
        out = out + lax.rem(lax.div(me, bit) + lax.div(i, bit), 2) * bit
        bit *= 2
    return out


def exchange(buf, axis, n, me, i, send_sem, recv_sem, src=None):
    return pltpu.make_async_remote_copy(
        src_ref=buf.at[me] if src is None else src,
        dst_ref=buf.at[me],
        send_sem=send_sem.at[i],
        recv_sem=recv_sem.at[i],
        device_id={axis: partner(me, i, n)},
        device_id_type=pl.DeviceIdType.MESH,
    )


def arrival(buf, axis, n, me, i, send_sem, recv_sem):
    slot = partner(me, i, n)
    return pltpu.make_async_remote_copy(
        src_ref=buf.at[slot],
        dst_ref=buf.at[slot],
        send_sem=send_sem.at[i],
        recv_sem=recv_sem.at[i],
        device_id={axis: slot},
        device_id_type=pl.DeviceIdType.MESH,
    )


def kernel(
    dims,
    energies_ref, current_ref, previous_ref, beta_ref, index_ref,
    right_hbm, left_hbm, screened_hbm,
    last_ref, prior_ref, alphas_ref, betas_ref,
    right, left, screened, packs, first, later, final, dens, held, fields, directs,
    dfull, vec_ref, early_ref, coef_ref, applied_ref, energy_ref, choose_ref, acc,
    right_sem, left_sem, screened_sem,
    pack_s, pack_r, full_s, full_r, kdens_s, kdens_r, gdens_s, gdens_r, field_s, field_r,
    direct_s, direct_r, final_s, final_r,
):
    nkp, npw, kl, nv, bands, gs = dims
    rows = kl * nv
    total = rows * nkp
    entries = total // nv * bands
    kme = lax.axis_index("kpt")
    pme = lax.axis_index("pw")

    right_copy = pltpu.make_async_copy(right_hbm, right, right_sem)
    left_copy = pltpu.make_async_copy(left_hbm, left, left_sem)

    def screened_copy(i):
        chunk = partner(pme, i, npw)
        start = pl.multiple_of(chunk * gs, gs)
        return pltpu.make_async_copy(
            screened_hbm.at[:, :, pl.ds(start, gs)], screened.at[chunk], screened_sem.at[i]
        )

    right_copy.start()
    for i in range(npw):
        screened_copy(i).start()
    left_copy.start()

    barrier = pltpu.get_barrier_semaphore()
    for axis, n, me in (("kpt", nkp, kme), ("pw", npw, pme)):
        for i in range(1, n):
            pl.semaphore_signal(
                barrier, inc=1, device_id={axis: partner(me, i, n)},
                device_id_type=pl.DeviceIdType.MESH,
            )
    width = energies_ref.shape[1]
    per = LANES // width
    levels = energies_ref[...]
    block = jnp.concatenate(
        [current_ref[v] for v in range(nv)]
        + [previous_ref[v] for v in range(nv)]
        + [levels for v in range(nv)],
        axis=0,
    )
    turn_at = lax.rem(pme, per)
    packs[pme] = jnp.concatenate(
        [block * (turn_at == j).astype(jnp.float32) for j in range(per)], axis=1
    )
    pl.semaphore_wait(barrier, nkp - 1 + npw - 1)

    pending = []

    def send_all(buf, axis, n, me, ssem, rsem):
        for i in range(1, n):
            copy = exchange(buf, axis, n, me, i, ssem, rsem)
            copy.start()
            pending.append(copy)

    def wait_all(buf, axis, n, me, ssem, rsem):
        for i in range(1, n):
            arrival(buf, axis, n, me, i, ssem, rsem).wait_recv()

    send_all(packs, "pw", npw, pme, pack_s, pack_r)

    points = nkp * kl
    row = lax.broadcasted_iota(jnp.int32, (total, points), 0)
    col = lax.broadcasted_iota(jnp.int32, (total, points), 1)
    point = (row // rows) * kl + lax.rem(row, kl)
    spread = (point == col).astype(jnp.bfloat16)
    index = index_ref[...].astype(jnp.float32).astype(jnp.bfloat16)
    wide = jnp.dot(spread, index, preferred_element_type=jnp.float32).astype(jnp.bfloat16)
    wide = lax.dot_general(
        wide, spread, (((1,), (1,)), ((), ())), preferred_element_type=jnp.float32
    )
    chain_row = lax.rem(lax.broadcasted_iota(jnp.int32, (total, total), 0), rows) // kl
    chain_col = lax.rem(lax.broadcasted_iota(jnp.int32, (total, total), 1), rows) // kl
    same = (chain_row == chain_col).astype(jnp.float32)
    for q in range(kl):
        transfer = (kme * kl + q).astype(jnp.float32)
        choose_ref[q * total : (q + 1) * total, :] = (
            same * jnp.maximum(1.0 - jnp.abs(wide - transfer), 0.0)
        ).astype(jnp.bfloat16)

    wait_all(packs, "pw", npw, pme, pack_s, pack_r)

    whole = jnp.concatenate(
        [sum(packs[m * per + j] for j in range(per)) for m in range(bands // LANES)], axis=1
    )
    vec_ref[...] = whole[:rows]
    early_ref[...] = whole[rows : 2 * rows]
    energy_ref[...] = whole[2 * rows :]
    coef_ref[...] = jnp.zeros_like(coef_ref)

    row_g = lax.broadcasted_iota(jnp.int32, (rows, gs), 0)
    row_g = lax.rem(row_g, kl)
    row_c = lax.rem(lax.broadcasted_iota(jnp.int32, (rows, bands), 0), kl)
    row_v = lax.broadcasted_iota(jnp.int32, (rows, LANES), 0) // kl
    lane = lax.broadcasted_iota(jnp.int32, (rows, LANES), 1)

    def densities(x):
        high = x.astype(jnp.bfloat16).astype(jnp.float32)
        both = jnp.concatenate([high, x - high], axis=0).astype(jnp.bfloat16)
        top = jnp.zeros((rows, gs), jnp.float32)
        low = jnp.zeros((rows, gs), jnp.float32)
        for k in range(kl):
            res = jnp.dot(both, right[k], preferred_element_type=jnp.float32)
            top = jnp.where(row_g == k, res[:rows], top)
            low = jnp.where(row_g == k, res[rows:], low)
        return top, low

    def sums_tile(vec, applied):
        cross = jnp.sum(vec * applied, axis=1, keepdims=True)
        square = jnp.sum(applied * applied, axis=1, keepdims=True)
        own = jnp.sum(vec * vec, axis=1, keepdims=True)
        return jnp.where(lane == 0, cross, jnp.where(lane == 1, square, own))

    def coefficients(tile, turn):
        sums = jnp.zeros_like(tile)
        for v in range(nv):
            chain = jnp.sum(jnp.where(row_v == v, tile, 0.0), axis=0, keepdims=True)
            sums = jnp.where(row_v == v, chain, sums)
        alpha = sums[:, 0:1] / entries
        mean = sums[:, 1:2] / entries - 2.0 * alpha * alpha + alpha * alpha * (sums[:, 2:3] / entries)
        beta = jnp.sqrt(mean + epsilon)
        coef = jnp.where(lane == turn, alpha, coef_ref[...])
        coef_ref[...] = jnp.where(lane == STEPS + turn, beta, coef)
        return alpha, beta

    def advance(alpha, beta):
        vec = vec_ref[...]
        early_ref[...] = vec
        vec_ref[...] = (applied_ref[...] - alpha * vec) / beta

    beta_before = jnp.zeros((rows, 1), jnp.float32)
    for v in range(nv):
        beta_before = jnp.where(row_v[:, 0:1] == v, beta_ref[v], beta_before)
    right_copy.wait()
    for turn in range(STEPS):
        if turn == 0:
            top, low = densities(vec_ref[...])
            first[kme] = top.astype(jnp.bfloat16)
            send_all(first, "kpt", nkp, kme, kdens_s.at[turn], kdens_r.at[turn])
            dfull[kme] = top + low
            wait_all(first, "kpt", nkp, kme, kdens_s.at[turn], kdens_r.at[turn])
            blocks = [first[s].astype(jnp.float32) for s in range(nkp)]
        else:
            applied = applied_ref[...]
            top, low = densities(applied)
            mine = later.at[turn - 1]
            mine[kme] = jnp.concatenate([top + low, sums_tile(vec_ref[...], applied)], axis=1)
            send_all(mine, "kpt", nkp, kme, kdens_s.at[turn], kdens_r.at[turn])
            wait_all(mine, "kpt", nkp, kme, kdens_s.at[turn], kdens_r.at[turn])
            if turn == 1:
                wait_all(dfull, "kpt", nkp, kme, full_s, full_r)
                for copy in full_copies:
                    copy.wait_send()
            alpha, beta = coefficients(sum(mine[s][:, gs:] for s in range(nkp)), turn - 1)
            blocks = []
            for s in range(nkp):
                block = (mine[s][:, :gs] - alpha * dfull[s]) / beta
                dfull[s] = block
                blocks.append(block)
        gathered = dens.at[turn]
        gathered[pme] = jnp.concatenate(blocks, axis=0).astype(jnp.bfloat16)
        gsend, grecv = gdens_s.at[turn], gdens_r.at[turn]
        for i in [1] + list(range(2, npw, 2)):
            copy = exchange(gathered, "pw", npw, pme, i, gsend, grecv)
            copy.start()
            pending.append(copy)
        if turn == 0:
            full_copies = []
            for i in range(1, nkp):
                copy = exchange(dfull, "kpt", nkp, kme, i, full_s, full_r)
                copy.start()
                full_copies.append(copy)
        if turn > 0:
            advance(alpha, beta)
            beta_before = beta
        acc[...] = jnp.zeros_like(acc)

        def product(i):
            if turn == 0:
                screened_copy(i).wait()
            chunk = partner(pme, i, npw)
            picked = jnp.dot(
                choose_ref[...], gathered[chunk], preferred_element_type=jnp.float32
            ).astype(jnp.bfloat16)
            part = acc[...]
            for q in range(kl):
                part = part + lax.dot_general(
                    picked[q * total : (q + 1) * total],
                    screened[chunk, q],
                    (((1,), (1,)), ((), ())),
                    preferred_element_type=jnp.float32,
                )
            acc[...] = part

        def forward(i):
            slot = partner(pme, i, npw)
            return pltpu.make_async_remote_copy(
                src_ref=gathered.at[slot],
                dst_ref=gathered.at[slot],
                send_sem=gsend.at[i + 1],
                recv_sem=grecv.at[i + 1],
                device_id={"pw": partner(pme, 1, npw)},
                device_id_type=pl.DeviceIdType.MESH,
            )

        def near_step(p, carry):
            i = 2 * p
            arrival(gathered, "pw", npw, pme, i, gsend, grecv).wait_recv()
            forward(i).start()
            product(i)
            return carry

        def far_step(p, carry):
            i = 2 * p + 1
            arrival(gathered, "pw", npw, pme, i, gsend, grecv).wait_recv()
            product(i)
            return carry

        product(0)
        far_step(0, 0)
        lax.fori_loop(1, npw // 2, near_step, 0)
        lax.fori_loop(1, npw // 2, far_step, 0)
        pending += [forward(i) for i in range(2, npw, 2)]
        out = held.at[turn]
        for s in range(nkp):
            out[s] = acc[s * rows : (s + 1) * rows, :].astype(jnp.bfloat16)
        mine = fields.at[turn]
        for i in range(1, nkp):
            copy = exchange(
                mine, "kpt", nkp, kme, i, field_s.at[turn], field_r.at[turn],
                src=out.at[partner(kme, i, nkp)],
            )
            copy.start()
            pending.append(copy)
        mine[kme] = out[kme]
        if turn == 0:
            left_copy.wait()
        wait_all(mine, "kpt", nkp, kme, field_s.at[turn], field_r.at[turn])
        field = sum(mine[s].astype(jnp.float32) for s in range(nkp)).astype(jnp.bfloat16)
        part = jnp.zeros((rows, bands), jnp.float32)
        for k in range(kl):
            res = lax.dot_general(
                field, left[k], (((1,), (1,)), ((), ())), preferred_element_type=jnp.float32
            )
            part = jnp.where(row_c == k, res, part)
        mine = directs.at[turn]
        mine[pme] = part.astype(jnp.bfloat16)
        send_all(mine, "pw", npw, pme, direct_s.at[turn], direct_r.at[turn])
        wait_all(mine, "pw", npw, pme, direct_s.at[turn], direct_r.at[turn])
        direct = sum(mine[s].astype(jnp.float32) for s in range(npw))
        applied_ref[...] = (
            energy_ref[...] * vec_ref[...] - direct - beta_before * early_ref[...]
        )
    final[kme] = sums_tile(vec_ref[...], applied_ref[...])
    send_all(final, "kpt", nkp, kme, final_s, final_r)
    wait_all(final, "kpt", nkp, kme, final_s, final_r)
    alpha, beta = coefficients(sum(final[s] for s in range(nkp)), STEPS - 1)
    advance(alpha, beta)
    for source, target in ((vec_ref, last_ref), (early_ref, prior_ref)):
        own = jnp.zeros((rows, width), jnp.float32)
        for m in range(npw):
            own = jnp.where(pme == m, source[:, m * width : (m + 1) * width], own)
        for v in range(nv):
            target[v] = own[v * kl : (v + 1) * kl]
    for v in range(nv):
        alphas_ref[v : v + 1, :] = coef_ref[v * kl : v * kl + 1, :STEPS]
        betas_ref[v : v + 1, :] = coef_ref[v * kl : v * kl + 1, STEPS : 2 * STEPS]
    for copy in pending:
        copy.wait_send()


def on_device(
    nkp, npw,
    energies, current, previous, previous_beta, pair_left, pair_right, screened, momentum_index
):
    nv, kl, width = current.shape
    bands = pair_left.shape[1]
    gs = pair_left.shape[2]
    qcount = screened.shape[0]
    rows = kl * nv
    total = rows * nkp
    f32, bf16 = jnp.float32, jnp.bfloat16
    vmem = pl.BlockSpec(memory_space=pltpu.VMEM)
    hbm = pl.BlockSpec(memory_space=pltpu.HBM)
    smem = pl.BlockSpec(memory_space=pltpu.SMEM)
    dma = pltpu.SemaphoreType.DMA
    return pl.pallas_call(
        functools.partial(kernel, (nkp, npw, kl, nv, bands, gs)),
        out_shape=(
            jax.ShapeDtypeStruct(current.shape, f32),
            jax.ShapeDtypeStruct(current.shape, f32),
            jax.ShapeDtypeStruct((nv, STEPS), f32),
            jax.ShapeDtypeStruct((nv, STEPS), f32),
        ),
        in_specs=[vmem, vmem, vmem, smem, vmem, hbm, hbm, hbm],
        out_specs=(vmem, vmem, vmem, vmem),
        scratch_shapes=[
            pltpu.VMEM((kl, bands, gs), bf16),
            pltpu.VMEM((kl, bands, gs), bf16),
            pltpu.VMEM((npw, qcount, gs, gs), bf16),
            pltpu.VMEM((npw, 3 * rows, LANES), f32),
            pltpu.VMEM((nkp, rows, gs), bf16),
            pltpu.VMEM((STEPS - 1, nkp, rows, gs + LANES), f32),
            pltpu.VMEM((nkp, rows, LANES), f32),
            pltpu.VMEM((STEPS, npw, total, gs), bf16),
            pltpu.VMEM((STEPS, nkp, rows, gs), bf16),
            pltpu.VMEM((STEPS, nkp, rows, gs), bf16),
            pltpu.VMEM((STEPS, npw, rows, bands), bf16),
            pltpu.VMEM((nkp, rows, gs), f32),
            pltpu.VMEM((rows, bands), f32),
            pltpu.VMEM((rows, bands), f32),
            pltpu.VMEM((rows, LANES), f32),
            pltpu.VMEM((rows, bands), f32),
            pltpu.VMEM((rows, bands), f32),
            pltpu.VMEM((qcount * total, total), bf16),
            pltpu.VMEM((total, gs), f32),
            dma, dma, dma((npw,)),
            dma((npw,)), dma((npw,)),
            dma((nkp,)), dma((nkp,)),
            dma((STEPS, nkp)), dma((STEPS, nkp)),
            dma((STEPS, npw)), dma((STEPS, npw)),
            dma((STEPS, nkp)), dma((STEPS, nkp)),
            dma((STEPS, npw)), dma((STEPS, npw)),
            dma((nkp,)), dma((nkp,)),
        ],
        compiler_params=pltpu.CompilerParams(
            collective_id=0, has_side_effects=True, vmem_limit_bytes=60 * 1024 * 1024
        ),
    )(
        energies, current, previous, previous_beta, momentum_index,
        pair_right, pair_left, screened,
    )


def solution(mesh):
    return jax.shard_map(
        functools.partial(on_device, mesh.shape["kpt"], mesh.shape["pw"]),
        mesh=mesh,
        in_specs=(
            P("kpt", "pw"),
            P(None, "kpt", "pw"),
            P(None, "kpt", "pw"),
            P(),
            P("kpt", None, "pw"),
            P("kpt", None, "pw"),
            P("kpt", "pw", None),
            P(),
        ),
        out_specs=(P(None, "kpt", "pw"), P(None, "kpt", "pw"), P(), P()),
        check_vma=False,
    )
```
